64 devices in a mesh: dp: 4 (over x, y), dcp: 16 (over z, core).
Axes of the slice: x: 2, y: 2, z: 8, core: 2. Of those that a mesh axis runs over, the one named last changes fastest.
The devices are a block of a 4x4x8 slice.
Arguments:
- q_abs: bfloat16 [64, 128, 576], P('dp', 'dcp'), parts along dimension 0
- cache: bfloat16 [64, 16384, 576], P('dp', 'dcp'), parts along dimension 0
- lengths: int32 [64], P('dp'), parts along dimension 0
Outputs:
- output: bfloat16 [64, 128, 512], P('dp', 'dcp'), parts along dimension 0
There are 4 independent parts. The reference program is written for one: setup_inputs(seed, part) draws one part's arguments, and reference() takes and returns one part's arrays. A program takes and returns all parts, laid end to end along the dimension named above; each array names one.
All inputs are finite; a program needn't handle non-finite values.
Results may differ from the reference program's by a relative error of at most 0.00794391.
Values are sent between devices in bfloat16 or wider.
A program may use at most 768 MiB of HBM per device.

```python
import jax
import jax.numpy as jnp
from jax import lax

HEADS = 128
KV_RANK = 512
ROPE = 64
QK_NOPE = 128
B = 16
S = 16384
NDEV = 16

WIDTH = KV_RANK + ROPE
SCALE = (QK_NOPE + ROPE) ** -0.5
BLOCK = S // NDEV
SEG = S // 32


def setup_inputs(seed: int = 0, part: int = 0) -> dict:
    key = jax.random.fold_in(jax.random.key(seed), part)
    kq, kc, kf, ks = jax.random.split(key, 4)
    q_abs = (jax.random.normal(kq, (B, HEADS, WIDTH), jnp.float32) * 0.6).astype(jnp.bfloat16)

    def draw(k):
        k1, k2, k3 = jax.random.split(k, 3)
        seg = jax.random.normal(k1, (32, KV_RANK), jnp.float32)
        lat = jax.random.normal(k2, (S, KV_RANK), jnp.float32) + jnp.repeat(seg, SEG, axis=0)
        rope = jax.random.normal(k3, (S, ROPE), jnp.float32) * 3.0
        return jnp.concatenate([lat, rope], axis=1).astype(jnp.bfloat16)

    cache = lax.map(draw, jax.random.split(kc, B))
    full = S - jax.random.randint(kf, (B,), 0, S // 64)
    short = jax.random.randint(ks, (B,), 1, S + 1)
    lengths = jnp.where(jnp.arange(B) % 2 == 0, full, short).astype(jnp.int32)
    return {'q_abs': q_abs, 'cache': cache, 'lengths': lengths}


def reference(q_abs, cache, lengths):
    pos = jnp.arange(S).reshape(NDEV, BLOCK)

    def one(args):
        qb, cb, lb = args
        cf = cb.astype(jnp.float32).reshape(NDEV, BLOCK, WIDTH)
        s = jnp.einsum('hk,ntk->nht', qb.astype(jnp.float32), cf) * SCALE
        valid = pos < lb
        s = jnp.where(valid[:, None, :], s, -jnp.inf)
        m = jnp.max(s, axis=2)
        m0 = jnp.where(jnp.isfinite(m), m, 0.0)
        p = jnp.exp(s - m0[:, :, None])
        l = jnp.sum(p, axis=2)
        pb = p.astype(jnp.bfloat16).astype(jnp.float32)
        pv = jnp.einsum('nht,ntc->nhc', pb, cf[:, :, :KV_RANK])
        has = l > 0.0
        l1 = jnp.where(has, l, 1.0)
        od = (pv / l1[:, :, None]).astype(jnp.bfloat16).astype(jnp.float32)
        lse_d = jnp.where(has, m0 + jnp.log(l1), -jnp.inf)
        mx = jnp.max(lse_d, axis=0)
        lse = mx + jnp.log(jnp.sum(jnp.exp(lse_d - mx[None, :]), axis=0))
        o = jnp.sum(jnp.exp(lse_d - lse[None, :])[:, :, None] * od, axis=0)
        return o.astype(jnp.bfloat16)

    return lax.map(one, (q_abs, cache, lengths))
```

```python
import functools

import jax
import jax.numpy as jnp
from jax import lax
from jax.experimental import pallas as pl
from jax.experimental.pallas import tpu as pltpu
from jax.sharding import PartitionSpec as P

ROPE = 64
SCALE = 192 ** -0.5
PAIR = 2
PIECE = 4
SKEW = 2
LANES = 128


def weights(lse):
    m = functools.reduce(jnp.maximum, lse)
    m = jnp.where(m == -jnp.inf, 0.0, m)
    w = [jnp.exp(x - m) for x in lse]
    t = functools.reduce(jnp.add, w)
    has = t > 0.0
    t1 = jnp.where(has, t, 1.0)
    inv = 1.0 / t1
    return [x * inv for x in w], jnp.where(has, m + jnp.log(t1), -jnp.inf)


def blend(parts, ws):
    reps = parts[0].shape[1] // LANES
    return functools.reduce(jnp.add, [x * jnp.concatenate([w] * reps, axis=1) for x, w in zip(parts, ws)])


def kernel(n, len_ref, q_ref, ct_ref, o_ref, ct, qall, own, sout, sin, lbuf, sbuf,
           csem, qsem, ags, agr, ds, dr, xs, xr, ls, lr, ss, sr):
    me = lax.axis_index('dcp')
    z, core = me // 2, me % 2
    chips = n // 2
    far, near = chips // 2, chips - 1 - chips // 2
    b, hl, wd = q_ref.shape
    sl = ct_ref.shape[2]
    lat = wd - ROPE
    groups, pieces = b // PAIR, b // PIECE
    rows = chips * hl

    def dev(off):
        return {'dcp': lax.rem(z + off + chips, chips) * 2 + core}

    sib = {'dcp': z * 2 + 1 - core}

    def remote(src, dst, s, r, to):
        return pltpu.make_async_remote_copy(src, dst, s, r, device_id=to, device_id_type=pl.DeviceIdType.MESH)

    qcopy = pltpu.make_async_copy(q_ref, qall.at[0, 0], qsem)
    qcopy.start()

    def cache_copy(s):
        return pltpu.make_async_copy(ct_ref.at[s], ct.at[s], csem.at[s])

    @pl.loop(0, b)
    def _(s):
        cache_copy(s).start()

    bar = pltpu.get_barrier_semaphore()
    for to in (dev(1), dev(-1), sib):
        pl.semaphore_signal(bar, inc=1, device_id=to, device_id_type=pl.DeviceIdType.MESH)
    pl.semaphore_wait(bar, 3)
    qcopy.wait()

    def q_at(half, r, p):
        return qall.at[half, r % chips, pl.ds(p * PIECE, PIECE)]

    def ring_q(p, k, long):
        sg = 1 if (p % 2 == 0) == long else -1
        i = k if long else far + k
        return remote(q_at(0, -k * sg, p), q_at(0, -(k + 1) * sg, p), ags.at[p, i], agr.at[p, i], dev(sg))

    def sib_q(p, r):
        return remote(q_at(0, r, p), q_at(1, r, p), ds.at[p, r % chips], dr.at[p, r % chips], sib)

    for p in range(pieces):
        ring_q(p, 0, True).start()
        ring_q(p, 0, False).start()
    for p in range(pieces):
        sib_q(p, 0).start()
    for k in range(1, far + 1):
        for p in range(pieces):
            for long in (True, False):
                hops = far if long else near
                if k <= hops:
                    sg = 1 if (p % 2 == 0) == long else -1
                    ring_q(p, k - 1, long).wait_recv()
                    if k < hops:
                        ring_q(p, k, long).start()
                    sib_q(p, -k * sg).start()
    for p in range(pieces):
        for r in range(chips):
            sib_q(p, r).wait_recv()

    base = me * sl

    def attend(s):
        cache_copy(s).wait()
        q = qall[:, :, s].reshape(2 * chips, hl, wd).astype(jnp.float32).reshape(2 * rows, wd).astype(jnp.bfloat16)
        sc = jnp.dot(q, ct[s], preferred_element_type=jnp.float32) * SCALE
        pos = base + lax.broadcasted_iota(jnp.int32, sc.shape, 1)
        sc = jnp.where(pos < len_ref[s], sc, -jnp.inf)
        m = jnp.max(sc, axis=1, keepdims=True)
        m0 = jnp.where(m == -jnp.inf, 0.0, m)
        p = jnp.exp(sc - m0)
        l = jnp.sum(p, axis=1, keepdims=True)
        pv = lax.dot_general(p.astype(jnp.bfloat16), ct[s, pl.ds(0, lat)], (((1,), (1,)), ((), ())),
                             preferred_element_type=jnp.float32)
        has = l > 0.0
        l1 = jnp.where(has, l, 1.0)
        od = (pv / l1).astype(jnp.bfloat16).astype(jnp.float32)
        lse = jnp.broadcast_to(jnp.where(has, m0 + jnp.log(l1), -jnp.inf), (2 * rows, LANES))
        own[s, :, pl.ds(0, lat)] = od[:rows]
        own[s, :, pl.ds(lat, LANES)] = lse[:rows]
        sout[s, :, pl.ds(0, lat)] = od[rows:]
        sout[s, :, pl.ds(lat, LANES)] = lse[rows:]

    def swap(g):
        return remote(sout.at[pl.ds(g * PAIR, PAIR)], sin.at[pl.ds(g * PAIR, PAIR)], xs.at[g], xr.at[g], sib)

    lane = lax.broadcasted_iota(jnp.int32, (hl, LANES), 1)

    def sign(g, long):
        odd = lax.rem(g, 2)
        return 1 - 2 * odd if long else 2 * odd - 1

    def chain(g, k, long):
        buf, s, r = (lbuf, ls, lr) if long else (sbuf, ss, sr)
        return remote(buf.at[g, k], buf.at[g, k + 1], s.at[g, k], r.at[g, k], dev(sign(g, long)))

    def mine(g, a, r):
        at = pl.ds(pl.multiple_of(lax.rem(r + chips, chips) * hl, hl), hl)
        return own[g * PAIR + a, at, pl.ds(0, lat)], own[g * PAIR + a, at, pl.ds(lat, LANES)]

    def unpack(buf, g, k, a):
        t = buf[g, k, :, pl.ds(PAIR * lat, LANES)]
        c = a * (LANES // PAIR)
        return buf[g, k, :, pl.ds(a * lat, lat)], jnp.broadcast_to(t[:, c:c + 1], (hl, LANES))

    def put(buf, g, k, parts):
        for a in range(PAIR):
            buf[g, k, :, pl.ds(a * lat, lat)] = parts[a][0]
        buf[g, k, :, pl.ds(PAIR * lat, LANES)] = jnp.where(lane < LANES // PAIR, parts[0][1], parts[1][1])

    def begin(g):
        swap(g).wait_recv()
        for a in range(PAIR):
            s = g * PAIR + a
            w, lse = weights([own[s, :, pl.ds(lat, LANES)], sin[s, :, pl.ds(lat, LANES)]])
            own[s, :, pl.ds(0, lat)] = blend([own[s, :, pl.ds(0, lat)], sin[s, :, pl.ds(0, lat)]], w)
            own[s, :, pl.ds(lat, LANES)] = lse
        for long, buf, hops in ((True, lbuf, far), (False, sbuf, near)):
            put(buf, g, 0, [mine(g, a, hops * sign(g, long)) for a in range(PAIR)])
            chain(g, 0, long).start()

    def hop(g, k, long):
        buf, hops = (lbuf, far) if long else (sbuf, near)
        chain(g, k - 1, long).wait_recv()
        parts = []
        for a in range(PAIR):
            x, y = unpack(buf, g, k, a), mine(g, a, (hops - k) * sign(g, long))
            w, lse = weights([x[1], y[1]])
            parts.append((blend([x[0], y[0]], w), lse))
        put(buf, g, k, parts)
        chain(g, k, long).start()

    def finish(g):
        chain(g, far - 1, True).wait_recv()
        chain(g, near - 1, False).wait_recv()
        for a in range(PAIR):
            x, y, v = unpack(lbuf, g, far, a), unpack(sbuf, g, near, a), mine(g, a, 0)
            w, _ = weights([x[1], y[1], v[1]])
            o_ref[g * PAIR + a] = blend([x[0], y[0], v[0]], w).astype(o_ref.dtype)

    def when(g, f):
        @pl.when(jnp.logical_and(g >= 0, g < groups))
        def _():
            f(g)

    @pl.loop(0, groups + 1 + SKEW * far)
    def _(i):
        when(i, lambda g: attend(g * PAIR))
        when(i - 1, begin)

        def rest(g):
            for a in range(1, PAIR):
                attend(g * PAIR + a)
            swap(g).start()

        when(i, rest)
        when(i - 1 - SKEW * far, finish)
        for k in range(far - 1, 0, -1):
            def step(g, k=k):
                hop(g, k, True)
                if k < near:
                    hop(g, k, False)
            when(i - 1 - SKEW * k, step)

    for p in range(pieces):
        for k in range(far):
            ring_q(p, k, True).wait_send()
        for k in range(near):
            ring_q(p, k, False).wait_send()
        for r in range(chips):
            sib_q(p, r).wait_send()

    @pl.loop(0, groups)
    def _(g):
        swap(g).wait_send()
        for k in range(far):
            chain(g, k, True).wait_send()
        for k in range(near):
            chain(g, k, False).wait_send()


def solution(mesh):
    n = mesh.shape['dcp']

    def local(q, cache, lengths):
        b, sl, wd = cache.shape
        hl = q.shape[1]
        lat = wd - ROPE
        chips = n // 2
        far, near = chips // 2, chips - 1 - chips // 2
        groups, pieces = b // PAIR, b // PIECE
        rows = chips * hl
        dma = pltpu.SemaphoreType.DMA
        return pl.pallas_call(
            functools.partial(kernel, n),
            out_shape=jax.ShapeDtypeStruct((b, hl, lat), jnp.bfloat16),
            in_specs=[pl.BlockSpec(memory_space=pltpu.SMEM), pl.BlockSpec(memory_space=pl.ANY),
                      pl.BlockSpec(memory_space=pl.ANY)],
            out_specs=pl.BlockSpec(memory_space=pltpu.VMEM),
            scratch_shapes=[
                pltpu.VMEM((b, wd, sl), jnp.bfloat16),
                pltpu.VMEM((2, chips, b, hl, wd), jnp.bfloat16),
                pltpu.VMEM((b, rows, lat + LANES), jnp.float32),
                pltpu.VMEM((b, rows, lat + LANES), jnp.float32),
                pltpu.VMEM((b, rows, lat + LANES), jnp.float32),
                pltpu.VMEM((groups, far + 1, hl, PAIR * lat + LANES), jnp.float32),
                pltpu.VMEM((groups, near + 1, hl, PAIR * lat + LANES), jnp.float32),
                dma((b,)), dma,
                dma((pieces, far + near)), dma((pieces, far + near)),
                dma((pieces, chips)), dma((pieces, chips)),
                dma((groups,)), dma((groups,)),
                dma((groups, far)), dma((groups, far)),
                dma((groups, near)), dma((groups, near)),
            ],
            compiler_params=pltpu.CompilerParams(
                collective_id=0, has_side_effects=True, vmem_limit_bytes=60 * 1024 * 1024),
            name='mla_decode',
        )(lengths, q, jnp.swapaxes(cache, 1, 2))

    return jax.shard_map(local, mesh=mesh, in_specs=(P('dp', 'dcp', None), P('dp', 'dcp', None), P('dp')),
                         out_specs=P('dp', 'dcp', None), check_vma=False)
```
